32 devices in a mesh: pole: 4 (over y, core), row: 2 (over x), col: 4 (over z).
Axes of the slice: x: 2, y: 2, z: 4, core: 2. Of those that a mesh axis runs over, the one named last changes fastest.
Arguments:
- l_factor: float32 [4, 2, 6, 512, 6, 512], P('pole', None, None, 'row', None, 'col'), may hold values from -0.21875 to 0.21875
- dinv: float32 [4, 2, 6, 512, 512], P('pole', None, None, 'row', 'col'), may hold values from -8 to 8, as said below
- weights: float32 [4, 2], P('pole'), may hold values from -4 to 4
- tiles: int32 [6, 24], replicated, may hold values 0 or 1
Outputs:
- density: float32 [6, 2, 256, 6, 512], P(None, 'row', 'pole', None, 'col')
The draws below stay inside these ranges and needn't reach their ends.
Inputs may be any that keep to these rules, and one draw needn't show every extreme that they name: Each of dinv's blocks is a symmetric complex matrix.
All inputs are finite; a program needn't handle non-finite values.
Results may differ from the reference program's by a relative error of at most 0.00012.
Values sent between devices are 32-bit elements; how exact they have to be, the bound alone decides.
No kernel may reach another device: no remote copies, remote signals or barrier semaphores. Data moves between devices by JAX's collectives and lax.ppermute only.
A program may use at most 192 MiB of HBM per device.

```python
import jax
import jax.numpy as jnp
from jax import lax

W = 512
NS = 6
TILE = 128
POLES = 4
N_ROW = 2


def draw_dinv(key, part):
    first, second, third = jax.random.split(jax.random.fold_in(key, 17), 3)
    noise = jax.random.normal(first, (POLES, 2, NS, W, W), jnp.float32)
    sym = (noise + jnp.swapaxes(noise, 3, 4)) * (0.6 / (2.0 * W) ** 0.5)
    real_diag = jax.random.uniform(second, (POLES, NS, W), jnp.float32, 0.5, 1.5)
    imag_diag = jax.random.uniform(third, (POLES, NS, W), jnp.float32, -0.5, 0.5)
    eye = jnp.eye(W, dtype=jnp.float32)
    diag = jnp.stack([real_diag, imag_diag], axis=1)[..., None] * eye
    result = sym + diag
    return jnp.clip(result, -8.0, 8.0)


def touch_ends(values, stream_key, least, high):
    longest = values.shape.index(max(values.shape))
    spots = []
    for shift in (0, 1):
        where = [jax.random.randint(jax.random.fold_in(stream_key, axis), (), 0, length) for axis, length in enumerate(values.shape)]
        where[longest] = (where[longest] + shift) % values.shape[longest]
        spots.append(tuple(where))
    return values.at[spots[0]].set(least).at[spots[1]].set(high)


def steps_of(key, shape, shards, least, largest):
    level = 1.0
    for dim, blocks in shards:
        steps = jax.random.uniform(jax.random.fold_in(jax.random.fold_in(key, 6), dim), (blocks,), jnp.float32, least / len(shards), largest / len(shards))
        level = level * jnp.repeat(jnp.exp(steps), shape[dim] // blocks).reshape((-1,) + (1,) * (len(shape) - 1 - dim))
    return level


def centred(key, shape, deviation, limit, pieces=(), held_as=jnp.bfloat16):
    values = jax.random.normal(key, shape, jnp.float32) * deviation
    if len(pieces) > 0:
        values = steps_of(key, shape, pieces, -0.22, 0.18) * values
    return jnp.clip(values, min=-limit, max=limit).astype(held_as)


def setup_inputs(seed: int = 0) -> dict:
    streams_of = jax.random.split(jax.random.key(seed), 5)
    return {
        "l_factor": centred(streams_of[0], (POLES, 2, NS, W, NS, W), (NS * W // 4) ** -0.5, 0.21875, ((0, 4), (3, 2), (5, 4)), jnp.float32),
        "dinv": draw_dinv(jax.random.fold_in(streams_of[4], 71), 0),
        "weights": centred(streams_of[2], (POLES, 2), 1.0, 4.0, ((0, 4),), jnp.float32),
        "tiles": touch_ends((jax.random.randint(streams_of[3], (NS, NS * W // TILE), 0, 4) < 3).astype(jnp.int32), jax.random.fold_in(streams_of[3], 1), 0, 1),
    }


def cdot_t(left, right):
    dims = (((0,), (0,)), ((), ()))

    def single(first, second):
        return lax.dot_general(first, second, dims, precision=lax.Precision.HIGHEST, preferred_element_type=jnp.float32)

    real = single(left[0], right[0]) - single(left[1], right[1])
    imag = single(left[0], right[1]) + single(left[1], right[0])
    return jnp.stack([real, imag])


def reference(l_factor, dinv, weights, tiles):
    total = NS * W
    row_keep = jnp.repeat(tiles, TILE, axis=1)
    keep = jnp.repeat(row_keep, W, axis=0).T.astype(jnp.float32)

    def one_pole(carry, inputs):
        factor, diag_inv, weight = inputs
        lower = factor.reshape(2, total, total) * keep[None]
        inverse = jnp.zeros((2, total, total), jnp.float32)
        last = (NS - 1) * W
        inverse = inverse.at[:, last:, last:].set(diag_inv[:, NS - 1])
        for step in range(NS - 2, -1, -1):
            start = step * W
            after = (step + 1) * W
            panel = lower[:, after:, start:start + W]
            block = inverse[:, after:, after:]
            row_part = -cdot_t(panel, block)
            inverse = inverse.at[:, start:start + W, after:].set(row_part)
            column = jnp.swapaxes(row_part, 1, 2)
            inverse = inverse.at[:, after:, start:start + W].set(column)
            inverse = inverse.at[:, start:start + W, start:start + W].set(diag_inv[:, step] - cdot_t(panel, column))
        return carry + weight[0] * inverse[0] - weight[1] * inverse[1], None

    summed, unused = lax.scan(one_pole, jnp.zeros((total, total), jnp.float32), (l_factor, dinv, weights))
    return summed.reshape(NS, N_ROW, W // N_ROW, NS, W)
```

```python
import functools

import jax
import jax.numpy as jnp
from jax import lax
from jax.experimental import pallas as pl
from jax.experimental.pallas import tpu as pltpu
from jax.sharding import PartitionSpec as P


AXES = ("pole", "row", "col")
F32 = jnp.float32
BF16 = jnp.bfloat16
NN = (((1,), (0,)), ((), ()))
NT = (((1,), (1,)), ((), ()))


def split(value):
    high = value.astype(BF16)
    return high, (value - high.astype(F32)).astype(BF16)


def dot(left, right, dims):
    return lax.dot_general(left, right, dims, preferred_element_type=F32)


def slot_of(after):
    return after * (after + 1) // 2


def product(high, low, right_high, right_low, slot, dims):
    rows = high.shape[0]
    half = rows // 2
    both = jnp.concatenate([high, low], axis=0)
    parts = []
    for part in range(2):
        twice = dot(both, right_high[slot, part], dims)
        parts.append(twice[:rows] + twice[rows:] + dot(high, right_low[slot, part], dims))
    real = parts[0][:half] - parts[1][half:]
    imag = parts[0][half:] + parts[1][:half]
    return jnp.concatenate([real, imag], axis=0)


def select_rows(position, owned, width, right_high, right_low, slot, dims):
    line = lax.broadcasted_iota(jnp.int32, (owned, width), 1)
    want = lax.broadcasted_iota(jnp.int32, (owned, width), 0) + position
    pick = jnp.where(line == want, 1.0, 0.0).astype(BF16)
    return jnp.concatenate(
        [dot(pick, right_high[slot, part], dims) + dot(pick, right_low[slot, part], dims) for part in range(2)], axis=0
    )


def copy_pieces(pieces, stage, sems, place, first=0):
    copies = []
    rows, cols = pieces[0][1].shape[2:]
    for number, ((flip_row, flip_half, flip_low), piece) in enumerate(pieces):
        row = place(0) ^ flip_row
        column = (place(1) ^ flip_half) * 2 + (place(2) ^ flip_low)
        copies.append(
            pltpu.make_async_copy(
                piece,
                stage.at[:, :, pl.ds(pl.multiple_of(row * rows, rows), rows), pl.ds(pl.multiple_of(column * cols, cols), cols)],
                sems.at[first + number],
            )
        )
    for copy in copies:
        copy.start()
    return copies


def weighted(value, weight, half):
    return weight[0] * value[:half] - weight[1] * value[half:]


def put_density(out, index, value, quarters):
    cols = value.shape[1] // quarters
    for quarter in range(quarters):
        out[quarter, index] = value[:, quarter * cols : (quarter + 1) * cols]


def forward(column, nsup, owned, value, solved_high, solved_low, state_high, state_low):
    def store(source):
        high, low = split(value[source])
        solved_high[source] = high
        solved_low[source] = low

    def outer(source, carry):
        store(source)
        base = slot_of(nsup - 1 - source)

        def inner(target, carry):
            slot = base + target - source - 1
            value[target] = value[target] - product(
                solved_high[source], solved_low[source], state_high, state_low, slot, NT
            )
            return carry

        return lax.fori_loop(source + 1, nsup, inner, carry)

    lax.fori_loop(column + 1, nsup - 1, outer, 0)
    store(nsup - 1)


def backward(column, nsup, value, solved_high, solved_low, state_high, state_low, g_high, g_low):
    def outer(step, carry):
        target = nsup - 1 - step
        after = nsup - 1 - target
        base = slot_of(after)
        start = product(solved_high[target], solved_low[target], state_high, state_low, base + after, NN)

        def inner(source, total):
            return total - product(
                g_high[column, source], g_low[column, source], state_high, state_low, base + source - target - 1, NN
            )

        total = lax.fori_loop(target + 1, nsup, inner, start)
        value[target] = total
        high, low = split(total)
        g_high[column, target] = high
        g_low[column, target] = low
        return carry

    lax.fori_loop(0, nsup - 1 - column, outer, 0)


def split_stage(stage, state_high, state_low, base, count):
    rows = 128
    width = stage.shape[2]

    def body(step, carry):
        slot = step // (width // rows)
        row = pl.multiple_of((step % (width // rows)) * rows, rows)
        for part in range(2):
            high, low = split(stage[part, slot, pl.ds(row, rows), :])
            state_high[base + slot, part, pl.ds(row, rows), :] = high
            state_low[base + slot, part, pl.ds(row, rows), :] = low
        return carry

    lax.fori_loop(0, count * (width // rows), body, 0)


def run_copies(copies):
    for copy in copies:
        copy.start()
    for copy in copies:
        copy.wait()


def column_kernel(column, nsup, owned, flips, *refs):
    after = nsup - 1 - column
    first = after == 1
    base = 0 if first else slot_of(after)
    count = slot_of(after) + after + 1 - base
    refs = list(refs)
    place, weight = refs[:2]
    pieces = refs[2 : 2 + len(flips)]
    rest = refs[2 + len(flips) :]
    if first:
        out_high, out_low, out_g_high, out_g_low, density = rest[:5]
        rest = rest[5:]
    else:
        in_high, in_low, in_g_high, in_g_low, out_high, out_low, out_g_high, out_g_low, density = rest[:9]
        rest = rest[9:]
    state_high, state_low, stage, g_high, g_low, solved_high, solved_low, value, sems = rest
    width = stage.shape[2]
    quarters = density.shape[0]
    where = lambda axis: place[axis]
    copies = copy_pieces(list(zip(flips, pieces)), stage, sems, where)
    number = len(flips)
    loads = []
    if not first:
        loads = [
            pltpu.make_async_copy(in_high.at[pl.ds(0, base)], state_high.at[pl.ds(0, base)], sems.at[number]),
            pltpu.make_async_copy(in_low.at[pl.ds(0, base)], state_low.at[pl.ds(0, base)], sems.at[number + 1]),
            pltpu.make_async_copy(in_g_high.at[pl.ds(column + 1, after)], g_high.at[pl.ds(column + 1, after)], sems.at[number + 2]),
            pltpu.make_async_copy(in_g_low.at[pl.ds(column + 1, after)], g_low.at[pl.ds(column + 1, after)], sems.at[number + 3]),
        ]
        for load in loads:
            load.start()
    for copy in copies:
        copy.wait()
    split_stage(stage, state_high, state_low, base, count)
    stores = [
        pltpu.make_async_copy(state_high.at[pl.ds(base, count)], out_high.at[pl.ds(base, count)], sems.at[0]),
        pltpu.make_async_copy(state_low.at[pl.ds(base, count)], out_low.at[pl.ds(base, count)], sems.at[1]),
    ]
    for store in stores:
        store.start()
    for load in loads:
        load.wait()
    position = place[3] * owned
    own = slot_of(after)
    select = functools.partial(select_rows, position, owned, width, state_high, state_low)

    def fill(target, carry):
        value[target] = -select(own + target - column - 1, NT)
        return carry

    lax.fori_loop(column + 1, nsup, fill, 0)
    if first:
        last = select(0, NN)
        high, low = split(last)
        g_high[nsup - 1, nsup - 1] = high
        g_low[nsup - 1, nsup - 1] = low
        put_density(density, 2 * after + 1, weighted(last, weight, owned), quarters)
    forward(column, nsup, owned, value, solved_high, solved_low, state_high, state_low)
    backward(column, nsup, value, solved_high, solved_low, state_high, state_low, g_high, g_low)

    def emit(target, carry):
        put_density(density, target - column + after, weighted(value[target], weight, owned), quarters)
        return carry

    lax.fori_loop(column + 1, nsup, emit, 0)

    def row(target, total):
        def inner(source, total):
            return total - product(
                g_high[target, source], g_low[target, source], state_high, state_low, own + source - column - 1, NN
            )

        total = lax.fori_loop(column + 1, nsup, inner, total)
        high, low = split(total)
        g_high[target, column] = high
        g_low[target, column] = low
        put_density(density, target - column, weighted(total, weight, owned), quarters)

    row(column, select(own + after, NN))

    def others(target, carry):
        row(target, jnp.zeros((2 * owned, width), F32))
        return carry

    lax.fori_loop(column + 1, nsup, others, 0)
    number = len(flips)
    run_copies(
        [
            pltpu.make_async_copy(g_high.at[pl.ds(column, after + 1)], out_g_high.at[pl.ds(column, after + 1)], sems.at[number]),
            pltpu.make_async_copy(g_low.at[pl.ds(column, after + 1)], out_g_low.at[pl.ds(column, after + 1)], sems.at[number + 1]),
        ]
    )
    for store in stores:
        store.wait()


def first_kernel(nsup, owned, flips, *refs):
    after = nsup - 1
    refs = list(refs)
    place, weight = refs[:2]
    pieces = refs[2 : 2 + len(flips)]
    in_high, in_low, in_g_high, in_g_low, out_a_high, out_a_low, density = refs[2 + len(flips) : 9 + len(flips)]
    state_high, state_low, stage, g_high, g_low, solved_high, solved_low, value, a_high, a_low, sems = refs[9 + len(flips) :]
    rows, cols = pieces[0].shape[2:]
    quarters = density.shape[0]
    copies = []
    for number, ((flip_row, flip_half, _), piece) in enumerate(zip(flips, pieces)):
        row = place[0] ^ flip_row
        half = place[1] ^ flip_half
        copies.append(
            pltpu.make_async_copy(
                piece,
                stage.at[:, :, pl.ds(pl.multiple_of(row * rows, rows), rows), pl.ds(pl.multiple_of(half * cols, cols), cols)],
                sems.at[number],
            )
        )
    number = len(flips)
    slots = state_high.shape[0]
    loads = [
        pltpu.make_async_copy(in_high.at[pl.ds(0, slots)], state_high, sems.at[number]),
        pltpu.make_async_copy(in_low.at[pl.ds(0, slots)], state_low, sems.at[number + 1]),
        pltpu.make_async_copy(in_g_high.at[pl.ds(1, after)], g_high.at[pl.ds(1, after)], sems.at[number + 2]),
        pltpu.make_async_copy(in_g_low.at[pl.ds(1, after)], g_low.at[pl.ds(1, after)], sems.at[number + 3]),
    ]
    run_copies(copies + loads)
    position = place[0] * cols + place[4] * owned
    line = lax.broadcasted_iota(jnp.int32, (owned, 2 * cols), 1)
    want = lax.broadcasted_iota(jnp.int32, (owned, 2 * cols), 0) + position
    pick = jnp.where(line == want, 1.0, 0.0).astype(BF16)

    def fill(target, carry):
        parts = []
        for part in range(2):
            high, low = split(stage[part, target - 1])
            parts.append(dot(pick, high, NT) + dot(pick, low, NT))
        value[target] = -jnp.concatenate(parts, axis=0)
        return carry

    lax.fori_loop(1, nsup, fill, 0)
    forward(0, nsup, owned, value, solved_high, solved_low, state_high, state_low)
    backward(0, nsup, value, solved_high, solved_low, state_high, state_low, g_high, g_low)

    def emit(target, carry):
        put_density(density, target - 1, weighted(value[target], weight, owned), quarters)
        return carry

    lax.fori_loop(1, nsup, emit, 0)

    def weigh_all(step, carry):
        column = step // after
        target = step % after + 1
        total = g_high[column, target].astype(F32) + g_low[column, target].astype(F32)
        real = weight[0] * total[:owned] - weight[1] * total[owned:]
        imag = weight[0] * total[owned:] + weight[1] * total[:owned]
        high, low = split(real)
        a_high[target - 1, 0, pl.ds(pl.multiple_of(column * owned, owned), owned)] = high
        a_low[target - 1, 0, pl.ds(pl.multiple_of(column * owned, owned), owned)] = low
        high, low = split(-imag)
        a_high[target - 1, 1, pl.ds(pl.multiple_of(column * owned, owned), owned)] = high
        a_low[target - 1, 1, pl.ds(pl.multiple_of(column * owned, owned), owned)] = low
        return carry

    lax.fori_loop(0, nsup * after, weigh_all, 0)
    run_copies(
        [
            pltpu.make_async_copy(a_high, out_a_high, sems.at[0]),
            pltpu.make_async_copy(a_low, out_a_low, sems.at[1]),
        ]
    )


def last_kernel(nsup, owned, flips, *refs):
    refs = list(refs)
    place = refs[0]
    pieces = refs[1 : 1 + len(flips)]
    a_high, a_low, density, stage, total, sems = refs[1 + len(flips) :]
    quarters = density.shape[0]
    copies = copy_pieces(list(zip(flips, pieces)), stage, sems, lambda axis: place[axis])
    for copy in copies:
        copy.wait()
    total[...] = jnp.zeros_like(total)
    width = stage.shape[2]
    depth = 256

    def body(step, carry):
        slot = step // (2 * (width // depth))
        part = (step // (width // depth)) % 2
        row = pl.multiple_of((step % (width // depth)) * depth, depth)
        high, low = split(stage[part, slot, pl.ds(row, depth), :])
        left = a_high[slot, part, :, pl.ds(row, depth)]
        total[...] -= dot(left, high, NN) + dot(left, low, NN) + dot(a_low[slot, part, :, pl.ds(row, depth)], high, NN)
        return carry

    lax.fori_loop(0, stage.shape[1] * 2 * (width // depth), body, 0)
    for column in range(nsup):
        put_density(density, column, total[column * owned : (column + 1) * owned], quarters)


def any_specs(count):
    return [pl.BlockSpec(memory_space=pl.ANY)] * count


def vmem_spec():
    return pl.BlockSpec(memory_space=pltpu.VMEM)


def smem_spec():
    return pl.BlockSpec(memory_space=pltpu.SMEM)


def params():
    return pltpu.CompilerParams(vmem_limit_bytes=63 * 1024 * 1024)


def cost(units, moved):
    return pl.CostEstimate(flops=units, bytes_accessed=moved, transcendentals=0)


def fast(l_factor, dinv, weights, tiles):
    npole, nrow, ncol = (lax.axis_size(name) for name in AXES)
    lows = ncol // 2
    index = {name: lax.axis_index(name) for name in AXES}
    factor, diag_inv = l_factor[0], dinv[0]
    nsup, rows_here, cols_here = factor.shape[1], factor.shape[2], factor.shape[4]
    width = rows_here * nrow
    owned = width // (nrow * lows * 2)
    core, high, low, row = index["pole"] % 2, index["col"] // lows, index["col"] % lows, index["row"]
    pole_high = index["pole"] // 2

    def permute(value, target):
        pairs = []
        for p in range(npole):
            for r in range(nrow):
                for q in range(ncol):
                    tp, tr, tq = target(p, r, q)
                    pairs.append(((p * nrow + r) * ncol + q, (tp * nrow + tr) * ncol + tq))
        return lax.ppermute(value, AXES, pairs)

    def swap(value):
        return permute(value, lambda p, r, q: (p - p % 2 + q // lows, r, (p % 2) * lows + q % lows))

    def over_row(value):
        return permute(value, lambda p, r, q: (p, 1 - r, q))

    def over_low(value):
        return permute(value, lambda p, r, q: (p, r, q ^ 1))

    def over_core(value):
        return permute(value, lambda p, r, q: (p ^ 1, r, q))

    tile_rows = nsup * width // tiles.shape[1]
    expanded = jnp.repeat(tiles.reshape(nsup, nsup, -1), tile_rows, axis=2)
    keep = lax.dynamic_slice_in_dim(expanded, row * rows_here, rows_here, 2).astype(F32)
    chunks = {}
    for column in range(nsup - 2, -1, -1):
        blocks = [factor[:, column + 1 :, :, column, :] * keep[column, column + 1 :][None, :, :, None]]
        if column == nsup - 2:
            blocks = [diag_inv[:, nsup - 1 :]] + blocks
        if column > 0:
            blocks.append(diag_inv[:, column : column + 1])
        chunks[column] = jnp.concatenate(blocks, axis=1) if len(blocks) > 1 else blocks[0]
    weight = swap(weights)[0]
    diag_zero = lax.psum_scatter(
        weights[0, 0] * diag_inv[0, 0] - weights[0, 1] * diag_inv[1, 0], "pole", scatter_dimension=0, tiled=True
    )

    place = jnp.stack([row, core, low, (row * lows + low) * 2 + core, core]).astype(jnp.int32)

    pieces = {}
    for column in range(nsup - 2, -1, -1):
        own = swap(chunks[column])
        got = {(0, 0, 0): own}
        got[1, 0, 0] = over_row(own)
        got[0, 0, 1] = over_low(own)
        got[0, 1, 0] = over_core(own)
        got[1, 1, 0] = over_core(got[1, 0, 0])
        if column in ROUTE_LOW:
            got[1, 0, 1] = over_low(got[1, 0, 0])
        else:
            got[1, 0, 1] = over_row(got[0, 0, 1])
        got[0, 1, 1] = over_core(got[0, 0, 1])
        got[1, 1, 1] = over_core(got[1, 0, 1])
        pieces[column] = got

    flips = tuple(sorted(pieces[0]))
    quarters = ncol
    total_slots = slot_of(nsup - 1)
    block_bytes = 2 * width * width * 4
    state_shape = jax.ShapeDtypeStruct((total_slots, 2, width, width), BF16)
    g_shape = jax.ShapeDtypeStruct((nsup, nsup, 2 * owned, width), BF16)
    block_flops = 3 * 8 * owned * width * width
    state = None
    densities = {}
    for column in range(nsup - 2, 0, -1):
        after = nsup - 1 - column
        is_first = after == 1
        slots = slot_of(after) + after + 1
        count = slots - (0 if is_first else slot_of(after))
        blocks = 2 * after + 1 + (1 if is_first else 0)
        density_shape = jax.ShapeDtypeStruct((quarters, blocks, owned, cols_here), F32)
        units = after * (after - 1) // 2 + after + after * (after - 1) // 2 + after * (after + 1) + 2
        base_args = 2 + len(flips)
        results = pl.pallas_call(
            functools.partial(column_kernel, column, nsup, owned, flips),
            out_shape=(state_shape, state_shape, g_shape, g_shape, density_shape),
            in_specs=[smem_spec(), smem_spec()] + any_specs(len(flips) + (0 if is_first else 4)),
            out_specs=tuple(any_specs(4)) + (vmem_spec(),),
            scratch_shapes=[
                pltpu.VMEM((slots, 2, width, width), BF16),
                pltpu.VMEM((slots, 2, width, width), BF16),
                pltpu.VMEM((2, count, width, width), F32),
                pltpu.VMEM((nsup, nsup, 2 * owned, width), BF16),
                pltpu.VMEM((nsup, nsup, 2 * owned, width), BF16),
                pltpu.VMEM((nsup, 2 * owned, width), BF16),
                pltpu.VMEM((nsup, 2 * owned, width), BF16),
                pltpu.VMEM((nsup, 2 * owned, width), F32),
                pltpu.SemaphoreType.DMA((len(flips) + 4,)),
            ],
            input_output_aliases={} if is_first else {base_args + i: i for i in range(4)},
            compiler_params=params(),
            cost_estimate=cost(units * block_flops, slots * block_bytes),
            name=f"column_{column}",
        )(place, weight, *[pieces[column][flip] for flip in flips], *([] if is_first else state))
        state = results[:4]
        densities[column] = results[4]

    near = tuple(flip for flip in flips if flip[2] == 0)
    slots = total_slots
    a_shape = jax.ShapeDtypeStruct((nsup - 1, 2, nsup * owned, width), BF16)
    a_high, a_low, densities["zero"] = pl.pallas_call(
        functools.partial(first_kernel, nsup, owned, near),
        out_shape=(a_shape, a_shape, jax.ShapeDtypeStruct((quarters, nsup - 1, owned, cols_here), F32)),
        in_specs=[smem_spec(), smem_spec()] + any_specs(len(near) + 4),
        out_specs=tuple(any_specs(2)) + (vmem_spec(),),
        scratch_shapes=[
            pltpu.VMEM((slots, 2, width, width), BF16),
            pltpu.VMEM((slots, 2, width, width), BF16),
            pltpu.VMEM((2, nsup - 1, width, 2 * cols_here), F32),
            pltpu.VMEM((nsup, nsup, 2 * owned, width), BF16),
            pltpu.VMEM((nsup, nsup, 2 * owned, width), BF16),
            pltpu.VMEM((nsup, 2 * owned, width), BF16),
            pltpu.VMEM((nsup, 2 * owned, width), BF16),
            pltpu.VMEM((nsup, 2 * owned, width), F32),
            pltpu.VMEM(a_shape.shape, BF16),
            pltpu.VMEM(a_shape.shape, BF16),
            pltpu.SemaphoreType.DMA((len(near) + 4,)),
        ],
        compiler_params=params(),
        cost_estimate=cost(30 * block_flops, slots * block_bytes),
        name="column_0",
    )(place, weight, *[pieces[0][flip] for flip in near], *state)

    densities["row"] = pl.pallas_call(
        functools.partial(last_kernel, nsup, owned, flips),
        out_shape=jax.ShapeDtypeStruct((quarters, nsup, owned, cols_here), F32),
        in_specs=[smem_spec()] + any_specs(len(flips)) + [vmem_spec(), vmem_spec()],
        out_specs=vmem_spec(),
        scratch_shapes=[
            pltpu.VMEM((2, nsup - 1, width, width), F32),
            pltpu.VMEM((nsup * owned, width), F32),
            pltpu.SemaphoreType.DMA((len(flips),)),
        ],
        compiler_params=params(),
        cost_estimate=cost(15 * block_flops, 5 * block_bytes),
        name="row_0",
    )(place, *[pieces[0][flip] for flip in flips], a_high, a_low)

    def reduce_poles(density):
        blocks = density.shape[1]
        if npole // 2 == lows:
            density = density.reshape(2, lows, blocks, owned, cols_here)
            total = lax.dynamic_index_in_dim(density, pole_high, 1, keepdims=False)
            for shift in range(1, lows):
                sent = lax.dynamic_index_in_dim(density, (pole_high + shift) % lows, 1, keepdims=False)
                total += permute(sent, lambda p, r, q: ((p // 2 + shift) % lows * 2 + p % 2, r, q))
            mine = lax.dynamic_index_in_dim(total, high, 0, keepdims=False)
            sent = lax.dynamic_index_in_dim(total, 1 - high, 0, keepdims=False)
            total = mine + permute(sent, lambda p, r, q: (p, r, (1 - q // lows) * lows + q % lows))
            return permute(total, lambda p, r, q: (q % lows * 2 + p % 2, r, q // lows * lows + p // 2))
        slices = lows * 2
        slot = low * 2 + core
        whole = jnp.zeros((slices,) + density.shape, F32)
        whole = lax.dynamic_update_index_in_dim(whole, density, slot, 0)
        whole = lax.psum(whole, ("pole", "col"))
        whole = lax.dynamic_index_in_dim(whole, index["col"], 1, keepdims=False)
        whole = jnp.transpose(whole, (1, 0, 2, 3)).reshape(blocks, rows_here, cols_here)
        return lax.dynamic_slice_in_dim(whole, index["pole"] * (rows_here // npole), rows_here // npole, 1)

    out_rows = rows_here // npole
    early = reduce_poles(jnp.concatenate([densities[column] for column in range(nsup - 2, 0, -1)], axis=1))
    middle = reduce_poles(densities["zero"])
    tail = reduce_poles(densities["row"])
    out = jnp.zeros((nsup, out_rows, nsup, cols_here), F32)
    offset = 0
    for column in range(nsup - 2, 0, -1):
        after = nsup - 1 - column
        block = early[offset : offset + after + 1]
        out = out.at[column:, :, column, :].set(block)
        block = early[offset + after + 1 : offset + 2 * after + 1]
        out = out.at[column, :, column + 1 :, :].set(jnp.transpose(block, (1, 0, 2)))
        offset += 2 * after + 1
        if after == 1:
            out = out.at[nsup - 1, :, nsup - 1, :].set(early[offset])
            offset += 1
    out = out.at[0, :, 1:, :].set(jnp.transpose(middle, (1, 0, 2)))
    tail = tail.at[0].add(diag_zero)
    out = out.at[:, :, 0, :].set(tail)
    return out[:, None]


ROUTE_LOW = (0,)


def cdot_t(left, right):
    dims = (((0,), (0,)), ((), ()))

    def single(first, second):
        return lax.dot_general(first, second, dims, precision=lax.Precision.HIGHEST, preferred_element_type=F32)

    real = single(left[0], right[0]) - single(left[1], right[1])
    imag = single(left[0], right[1]) + single(left[1], right[0])
    return jnp.stack([real, imag])


def weigh(values, weight):
    return weight[0] * values[0] - weight[1] * values[1]


def general(l_factor, dinv, weights, tiles):
    nrow = lax.axis_size("row")
    npole = lax.axis_size("pole")
    row_index = lax.axis_index("row")
    factor = l_factor[0]
    diag_inv = dinv[0]
    weight = weights[0]
    nsup = factor.shape[1]
    rows_here = factor.shape[2]
    cols_here = factor.shape[4]
    width = rows_here * nrow
    tile_rows = nsup * width // tiles.shape[1]
    expanded = jnp.repeat(tiles.reshape(nsup, nsup, -1), tile_rows, axis=2)
    local_keep = lax.dynamic_slice_in_dim(expanded, row_index * rows_here, rows_here, 2)
    keep = jnp.transpose(local_keep, (1, 2, 0)).astype(F32)
    masked = factor * keep[None, :, :, :, None]
    inverse = jnp.zeros((2, nsup, rows_here, nsup, cols_here), F32)
    inverse = inverse.at[:, nsup - 1, :, nsup - 1, :].set(diag_inv[:, nsup - 1])
    for step in range(nsup - 2, -1, -1):
        span = nsup - 1 - step
        panel = lax.all_gather(masked[:, step + 1 :, :, step, :], "col", axis=3, tiled=True)
        panel_rows = panel.reshape(2, span * rows_here, width)
        block = inverse[:, step + 1 :, :, step + 1 :, :].reshape(2, span * rows_here, span * cols_here)
        row_full = lax.psum(-cdot_t(panel_rows, block), "row")
        row_mine = lax.dynamic_slice_in_dim(row_full, row_index * rows_here, rows_here, 1)
        inverse = inverse.at[:, step, :, step + 1 :, :].set(row_mine.reshape(2, rows_here, span, cols_here))
        swapped = lax.all_to_all(
            row_full.reshape(2, width, span, cols_here), "col", split_axis=1, concat_axis=3, tiled=True
        )
        mine = lax.dynamic_slice_in_dim(swapped, row_index * rows_here, rows_here, 3)
        column = jnp.transpose(mine, (0, 2, 3, 1))
        inverse = inverse.at[:, step + 1 :, :, step, :].set(column)
        correction = cdot_t(panel_rows, column.reshape(2, span * rows_here, cols_here))
        diag_share = lax.psum_scatter(correction, "row", scatter_dimension=1, tiled=True)
        inverse = inverse.at[:, step, :, step, :].set(diag_inv[:, step] - diag_share)
    summed = lax.psum_scatter(weigh(inverse, weight), "pole", scatter_dimension=1, tiled=True)
    return summed.reshape(nsup, 1, rows_here // npole, nsup, cols_here)


def solution(mesh):
    sizes = mesh.shape
    chosen = fast if sizes["row"] == 2 and sizes["col"] == 4 and sizes["pole"] % 2 == 0 else general
    return jax.shard_map(
        chosen,
        mesh=mesh,
        in_specs=(
            P("pole", None, None, "row", None, "col"),
            P("pole", None, None, "row", "col"),
            P("pole", None),
            P(),
        ),
        out_specs=P(None, "row", "pole", None, "col"),
        check_vma=False,
    )
```
